32 devices in a mesh: row: 4 (over x, core), col: 8 (over z, y).
Axes of the slice: x: 2, y: 2, z: 4, core: 2. Of those that a mesh axis runs over, the one named last changes fastest.
Arguments:
- ancestor_inv: bfloat16 [32, 32, 256, 256], P('row', 'col'), may hold values from -0.29882812 to 0.29882812
- lower_panel: bfloat16 [8, 16, 256, 256], P('row', 'col'), may hold values from -0.59765625 to 0.59765625
- upper_panel: bfloat16 [8, 16, 256, 256], P('col', 'row'), may hold values from -0.59765625 to 0.59765625
- pivot_inv: float32 [8, 256, 256], P('col'), may hold values from -6 to 6
- members: int32 [8, 16], replicated, may hold values from -1 to 31, as said below
Outputs:
- lower_inv: bfloat16 [8, 16, 256, 256], P('col', 'row')
- upper_inv: bfloat16 [8, 16, 256, 256], P('row', 'col')
- diag_inv: float32 [8, 256, 256], P('col')
The draws below stay inside these ranges and needn't reach their ends.
Inputs may be any that keep to these rules, and one draw needn't show every extreme that they name: `members`: slot s belongs to group g = s // 2; a used slot names an ancestor block of that group, from g * 4 to (g + 1) * 4 - 1. In each group of each supernode the used slots come first, name distinct blocks, and number 1 to 2; every group has 2 used slots for some supernode. Empty slots hold -1.
All inputs are finite; a program needn't handle non-finite values.
Results may differ from the reference program's by a relative error of at most 0.013.
Values may be sent and summed in bfloat16 or wider, within the bound.
A program may use at most 128 MiB of HBM per device.

```python
from functools import partial
import jax
import jax.numpy as jnp
from jax import lax

B = 256
NBC = 4
CAP = 2
KL = 8
NB = 32
SLOTS = 16


def draw_members(key, part):
    groups = SLOTS // CAP
    key_counts, key_fullrow, key_ranking = jax.random.split(key, 3)
    counts = jax.random.randint(key_counts, (KL, groups), 1, CAP + 1)
    full_row = jax.random.randint(key_fullrow, (groups,), 0, KL)
    counts = jnp.where(jnp.arange(KL)[:, None] == full_row[None, :], CAP, counts)
    scores = jax.random.randint(key_ranking, (KL, groups, NBC), 0, 1 << 20) * NBC + jnp.arange(NBC)[None, None, :]
    ranking = jnp.argsort(scores, axis=-1)[:, :, :CAP]
    blocks = ranking + (jnp.arange(groups) * NBC)[None, :, None]
    in_use = jnp.arange(CAP)[None, None, :] < counts[:, :, None]
    return jnp.where(in_use, blocks, -1).astype(jnp.int32).reshape(KL, SLOTS)


def steps_of(own_key, dims, pieces, least, largest):
    loudness = 1.0
    for dim, parts in pieces:
        heights = jax.random.uniform(jax.random.fold_in(jax.random.fold_in(own_key, 6), dim), (parts,), jnp.float32, least / len(pieces), largest / len(pieces))
        loudness = loudness * jnp.repeat(jnp.exp(heights), dims[dim] // parts).reshape((-1,) + (1,) * (len(dims) - 1 - dim))
    return loudness


def gaussian(stream_key, shape, spread, reach, shards=(), dtype=jnp.bfloat16):
    entries = spread * jax.random.normal(stream_key, shape, jnp.float32)
    if shards:
        entries = entries * steps_of(stream_key, shape, shards, -0.22, 0.18)
    return jnp.clip(entries, -reach, reach).astype(dtype)


def setup_inputs(seed: int = 0) -> dict:
    streams_of = jax.random.split(jax.random.key(seed), 6)
    return {
        "ancestor_inv": gaussian(streams_of[0], (NB, NB, B, B), 0.05, 0.29882812, ((0, 4), (1, 8))),
        "lower_panel": gaussian(streams_of[1], (KL, SLOTS, B, B), 0.1, 0.59765625, ((0, 4), (1, 8))),
        "upper_panel": gaussian(streams_of[2], (KL, SLOTS, B, B), 0.1, 0.59765625, ((0, 8), (1, 4))),
        "pivot_inv": gaussian(streams_of[3], (KL, B, B), 1.0, 6.0, ((0, 8),), jnp.float32),
        "members": draw_members(jax.random.fold_in(streams_of[5], 71), 0),
    }


def one_supernode(ancestor_inv, item):
    member_row, lower_blocks, upper_blocks, pivot_block = item
    valid = member_row >= 0
    chosen = jnp.where(valid, member_row, 0).astype(jnp.int32)
    strip = jnp.take(ancestor_inv, chosen, axis=0)
    square = jnp.take(strip, chosen, axis=1).astype(jnp.float32)
    weight = valid.astype(jnp.float32)[:, None, None]
    lower_masked = lower_blocks.astype(jnp.float32) * weight
    upper_masked = upper_blocks.astype(jnp.float32) * weight
    lower_sum = -jnp.einsum("ijab,jbc->iac", square, lower_masked) * weight
    lower_inv = lower_sum.astype(jnp.bfloat16)
    upper_sum = -jnp.einsum("iab,ijbc->jac", upper_masked, square) * weight
    upper_inv = upper_sum.astype(jnp.bfloat16)
    diag_inv = pivot_block - jnp.einsum("iab,ibc->ac", upper_masked, lower_inv.astype(jnp.float32))
    return lower_inv, upper_inv, diag_inv


def reference(ancestor_inv, lower_panel, upper_panel, pivot_inv, members):
    lower_inv, upper_inv, diag_inv = lax.map(partial(one_supernode, ancestor_inv), (members, lower_panel, upper_panel, pivot_inv))
    return (lower_inv, upper_inv, diag_inv)
```

```python
import functools

import jax
import jax.numpy as jnp
from jax import lax
from jax.experimental import pallas as pl
from jax.experimental.pallas import tpu as pltpu
from jax.sharding import PartitionSpec as P

NY = 2
CORES = 2
BF = jnp.bfloat16
F32 = jnp.float32


def kernel(
    n_row, n_col, nq, hp,
    mem, anc, low, upp, piv,
    low_out, upp_out, diag_out,
    a, lbuf, ubuf, pl_buf, yr, zr, pu, ur, ds, dr, acc, dacc,
    loc, l_s, l_rel, l_r, uy_s, uy_r, uz_s, uz_r, ry_s, ry_r, rz_s, rz_r, pu_s, pu_r, d_s, d_r,
):
    row = lax.axis_index("row")
    col = lax.axis_index("col")
    nz = n_col // NY
    nx = n_row // CORES
    x, core = row // CORES, row % CORES
    z, y = col // NY, col % NY
    yp = z * NY + (1 - y)
    rb, cb = anc.shape[0], anc.shape[1]
    kr, cs = low.shape[0], low.shape[1]
    rs = upp.shape[1]
    ny_blocks = rs - nq
    hb = rs // hp
    partner = x * CORES + (1 - core)

    def remote(src, dst, ss, rsem, **where):
        return pltpu.make_async_remote_copy(
            src_ref=src, dst_ref=dst, send_sem=ss, recv_sem=rsem, device_id=where
        )

    ca = pltpu.make_async_copy(anc, a, loc.at[0])
    cl = pltpu.make_async_copy(low, lbuf.at[pl.ds(row * kr, kr)], loc.at[1])
    cu = pltpu.make_async_copy(upp.at[0], ubuf.at[col], loc.at[2])
    cl.start()
    cu.start()
    ca.start()

    bar = pltpu.get_barrier_semaphore()
    for dx in range(1, n_row):
        pl.semaphore_signal(bar, inc=1, device_id={"row": (row + dx) % n_row})
    pl.semaphore_signal(bar, inc=1, device_id={"col": yp})

    @pl.when(z > 0)
    def _():
        pl.semaphore_signal(bar, inc=1, device_id={"col": col - NY})

    @pl.when(z < nz - 1)
    def _():
        pl.semaphore_signal(bar, inc=1, device_id={"col": col + NY})

    peers = n_row + jnp.where(z > 0, 1, 0) + jnp.where(z < nz - 1, 1, 0)
    pl.semaphore_wait(bar, peers)

    def l_own(r2):
        return remote(low, lbuf.at[pl.ds(row * kr, kr)], l_s.at[r2], l_r.at[row], row=r2)

    def l_recv(r2):
        blk = lbuf.at[pl.ds(r2 * kr, kr)]
        return remote(blk, blk, l_rel.at[r2], l_r.at[r2], row=partner)

    def uy_own(kind):
        part = pl.ds(0, ny_blocks) if kind else pl.ds(ny_blocks, nq)
        return remote(
            upp.at[0, part], ubuf.at[col, part], uy_s.at[nz if kind == 0 else z],
            uy_r.at[nz if kind == 0 else z], col=yp,
        )

    def uy_got(kind, zs):
        part = pl.ds(0, ny_blocks) if kind else pl.ds(ny_blocks, nq)
        blk = ubuf.at[zs * NY + (1 - y), part]
        return remote(blk, blk, uy_s.at[zs], uy_r.at[nz if kind == 0 else zs], col=yp)

    def uy_pass(zs):
        blk = ubuf.at[zs * NY + y, pl.ds(0, ny_blocks)]
        return remote(blk, blk, uy_s.at[zs], uy_r.at[zs], col=yp)

    def uz(zs, kind, up):
        if kind == 0:
            blk = ubuf.at[zs * NY + y]
        else:
            blk = ubuf.at[zs * NY + (1 - y), pl.ds(ny_blocks, nq)]
        to = col + NY if up else col - NY
        return remote(blk, blk, uz_s.at[zs, int(up), kind], uz_r.at[zs, kind], col=to)

    def uz_own(up):
        to = col + NY if up else col - NY
        return remote(upp.at[0], ubuf.at[col], uz_s.at[z, int(up), 0], uz_r.at[z, 0], col=to)

    def ry(zd, h):
        part = pl.ds(h * hb, hb)
        return remote(
            pl_buf.at[zd * NY + (1 - y), part], yr.at[zd, part], ry_s.at[zd, h], ry_r.at[zd, h],
            col=yp,
        )

    def rz(zd, h, up):
        part = pl.ds(h * hb, hb)
        slot = zd + 1 if up else zd
        to = col + NY if up else col - NY
        return remote(
            pl_buf.at[zd * NY + y, part], zr.at[slot, part], rz_s.at[zd, h], rz_r.at[slot, h],
            col=to,
        )

    def pu_copy(k):
        return remote(pu.at[k], ur.at[row, k % kr], pu_s.at[k], pu_r.at[row, k % kr], row=k // kr)

    def pu_got(r2, p):
        return remote(pu.at[0], ur.at[r2, p], pu_s.at[0], pu_r.at[r2, p], row=r2)

    def d_copy(r2):
        return remote(ds, dr.at[row], d_s.at[r2], d_r.at[row], row=r2)

    def d_got(r2):
        return remote(ds, dr.at[r2], d_s.at[r2], d_r.at[r2], row=r2)

    def each_dir(fn):
        @pl.when(z > 0)
        def _():
            fn(False)

        @pl.when(z < nz - 1)
        def _():
            fn(True)

    def row_member(k, i):
        m = mem[k, row * rs + i]
        return m >= 0, jnp.clip(m - row * rb, 0, rb - 1)

    def col_member(k, j):
        m = mem[k, col * cs + j]
        return m >= 0, jnp.clip(m - col * cb, 0, cb - 1)

    zero = jnp.zeros((), BF)

    def lower_part(k):
        cols = [col_member(k, j) for j in range(cs)]
        panels = [jnp.where(cols[j][0], lbuf[k, j], zero) for j in range(cs)]

        def one(i, _):
            ok, ri = row_member(k, i)
            tot = None
            for j in range(cs):
                t = jnp.dot(a[ri, cols[j][1]], panels[j], preferred_element_type=F32)
                tot = t if tot is None else tot + t
            pl_buf[k, i] = jnp.where(ok, tot, 0.0).astype(BF)
            return 0

        lax.fori_loop(0, rs, one, 0)

    def upper_part(k):
        rows = [row_member(k, i) for i in range(rs)]

        def one(j, _):
            ok, cj = col_member(k, j)
            tot = None
            for i in range(rs):
                t = jnp.dot(
                    jnp.where(rows[i][0], ubuf[k, i], zero), a[rows[i][1], cj],
                    preferred_element_type=F32,
                )
                tot = t if tot is None else tot + t
            pu[k, j] = jnp.where(ok, tot, 0.0).astype(BF)
            return 0

        lax.fori_loop(0, cs, one, 0)

        @pl.when(k // kr != row)
        def _():
            pu_copy(k).start()

    def lower_group(r2):
        def one(p, _):
            k = r2 * kr + (p + 1 - y) % NY
            lower_part(k)

            @pl.when(k % NY != y)
            def _():
                for h in range(hp):
                    ry(k // NY, h).start()

            return 0

        lax.fori_loop(0, kr, one, 0)

    l_own(partner).start()
    for dx in range(1, nx):
        l_own(((x + dx) % nx) * CORES + core).start()
    uy_own(0).start()
    each_dir(lambda up: uz_own(up).start())

    ca.wait()
    cl.wait()
    lower_group(row)
    l_recv(partner).wait_recv()
    lower_group(partner)

    uy_got(0, z).wait_recv()
    each_dir(lambda up: uz(z, 1, up).start())
    cu.wait()
    upper_part(col)

    def others(fn):
        for dx in range(1, nx):
            fn((x + dx) % nx)

    def relay(x2):
        l_recv(x2 * CORES + core).wait_recv()
        l_recv(x2 * CORES + core).start()

    others(relay)

    def by_side(d, fn):
        @pl.when(z - d >= 0)
        def _():
            fn(z - d, True)

        @pl.when(z + d <= nz - 1)
        def _():
            fn(z + d, False)

    def take(zs, up):
        for kind in range(2):
            uz(zs, kind, up).wait_recv()

            @pl.when((z < nz - 1) if up else (z > 0))
            def _():
                uz(zs, kind, up).start()

    by_side(1, take)

    def late(x2):
        lower_group(x2 * CORES + core)
        l_recv(x2 * CORES + 1 - core).wait_recv()
        lower_group(x2 * CORES + 1 - core)

    others(late)
    uy_own(1).start()
    by_side(1, lambda zs, up: uy_pass(zs).start())

    def near(d):
        def one(s, _):
            zs = z + (2 * s - 1) * d

            @pl.when(jnp.logical_and(zs >= 0, zs < nz))
            def _():
                upper_part(zs * NY + y)

            return 0

        lax.fori_loop(0, 2, one, 0)

    def far(d):
        def one(s, _):
            zs = z + (2 * s - 1) * d

            @pl.when(jnp.logical_and(zs >= 0, zs < nz))
            def _():
                uy_got(1, zs).wait_recv()
                upper_part(zs * NY + (1 - y))

            return 0

        lax.fori_loop(0, 2, one, 0)

    def band_sum(zd, t):
        k = zd * NY + y

        def go(up):
            def piece(h, _):
                part = pl.ds(h * hb, hb)
                ry(zd, h).wait_recv()

                @pl.when((z > 0) if up else (z < nz - 1))
                def _():
                    rz(zd, h, up).wait_recv()
                    slot = zd + 1 if up else zd
                    pl_buf[k, part] = (
                        pl_buf[k, part].astype(F32) + yr[zd, part].astype(F32)
                        + zr[slot, part].astype(F32)
                    ).astype(BF)

                @pl.when((z == 0) if up else (z == nz - 1))
                def _():
                    pl_buf[k, part] = (
                        pl_buf[k, part].astype(F32) + yr[zd, part].astype(F32)
                    ).astype(BF)

                rz(zd, h, up).start()
                return 0

            lax.fori_loop(0, hp, piece, 0)

        @pl.when(zd > z)
        def _():
            go(True)

        @pl.when(zd < z)
        def _():
            go(False)

    def chain(t):
        band_sum((CORES * x + t) % nz, t)

    near(1)
    chain(0)
    for d in range(2, nz):
        by_side(d, take)
        by_side(d, lambda zs, up: uy_pass(zs).start())
        near(d)
        chain(d - 1)
    uy_got(1, z).wait_recv()
    upper_part(yp)
    far(1)
    chain(nz - 1)

    def final(h, _):
        part = pl.ds(h * hb, hb)
        ry(z, h).wait_recv()
        acc[part] = pl_buf[col, part].astype(F32) + yr[z, part].astype(F32)

        @pl.when(z > 0)
        def _():
            rz(z, h, True).wait_recv()
            acc[part] = acc[part] + zr[z + 1, part].astype(F32)

        @pl.when(z < nz - 1)
        def _():
            rz(z, h, False).wait_recv()
            acc[part] = acc[part] + zr[z, part].astype(F32)

        low_out[0, part] = (-acc[part]).astype(BF)
        return 0

    lax.fori_loop(0, hp, final, 0)
    tot = None
    for i in range(rs):
        t = jnp.dot(
            jnp.where(row_member(col, i)[0], ubuf[col, i], zero), low_out[0, i],
            preferred_element_type=F32,
        )
        tot = t if tot is None else tot + t
    dacc[...] = tot
    ds[...] = tot.astype(BF)
    for dx in range(1, n_row):
        d_copy((row + dx) % n_row).start()

    lax.fori_loop(2, nz, lambda d, _: (far(d), 0)[1], 0)

    for dx in range(1, n_row):
        r2 = (row + dx) % n_row
        d_got(r2).wait_recv()
        dacc[...] = dacc[...] + dr[r2].astype(F32)
    diag_out[0] = piv[0] - dacc[...]

    for p in range(kr):
        for j in range(cs):
            acc[p * cs + j] = pu[row * kr + p, j].astype(F32)
    for dx in range(1, n_row):
        r2 = (row + dx) % n_row
        for p in range(kr):
            pu_got(r2, p).wait_recv()
            for j in range(cs):
                acc[p * cs + j] = acc[p * cs + j] + ur[r2, p, j].astype(F32)
    for p in range(kr):
        for j in range(cs):
            upp_out[p, j] = (-acc[p * cs + j]).astype(BF)

    l_own(partner).wait_send()
    for dx in range(1, nx):
        r2 = ((x + dx) % nx) * CORES + core
        l_own(r2).wait_send()
        l_recv(r2).wait_send()
    uy_own(0).wait_send()
    uy_own(1).wait_send()

    def own_done(up):
        uz_own(up).wait_send()
        uz(z, 1, up).wait_send()

    each_dir(own_done)

    def passed(zs, up):
        uy_pass(zs).wait_send()

        @pl.when((z < nz - 1) if up else (z > 0))
        def _():
            for kind in range(2):
                uz(zs, kind, up).wait_send()

    for d in range(1, nz):
        by_side(d, passed)

    def sums_done(zd, _):
        for h in range(hp):
            ry(zd, h).wait_send()

            @pl.when(zd > z)
            def _():
                rz(zd, h, True).wait_send()

            @pl.when(zd < z)
            def _():
                rz(zd, h, False).wait_send()

        return 0

    lax.fori_loop(0, nz, sums_done, 0)

    def parts_done(k, _):
        @pl.when(k // kr != row)
        def _():
            pu_copy(k).wait_send()

        return 0

    lax.fori_loop(0, n_col, parts_done, 0)
    for dx in range(1, n_row):
        d_copy((row + dx) % n_row).wait_send()


def body(ancestor_inv, lower_panel, upper_panel, pivot_inv, members):
    n_col = lax.axis_size("col")
    n_row = lax.axis_size("row")
    side = ancestor_inv.shape[2]
    rb, cb = ancestor_inv.shape[:2]
    kr, cs = lower_panel.shape[:2]
    per_col, rs = upper_panel.shape[:2]
    level = members.shape[0]
    nz = n_col // NY
    assert per_col == 1 and level == n_col and kr == NY and nz == n_row
    hp = 2
    nq = rs // 4
    blk = (side, side)
    dma = pltpu.SemaphoreType.DMA
    vmem = pl.BlockSpec(memory_space=pltpu.VMEM)
    hbm = pl.BlockSpec(memory_space=pltpu.HBM)
    return pl.pallas_call(
        functools.partial(kernel, n_row, n_col, nq, hp),
        out_shape=(
            jax.ShapeDtypeStruct((per_col, rs) + blk, BF),
            jax.ShapeDtypeStruct((kr, cs) + blk, BF),
            jax.ShapeDtypeStruct((per_col,) + blk, F32),
        ),
        in_specs=[pl.BlockSpec(memory_space=pltpu.SMEM), hbm, hbm, hbm, vmem],
        out_specs=(vmem, vmem, vmem),
        scratch_shapes=[
            pltpu.VMEM((rb, cb) + blk, BF),
            pltpu.VMEM((level, cs) + blk, BF),
            pltpu.VMEM((n_col, rs) + blk, BF),
            pltpu.VMEM((n_col, rs) + blk, BF),
            pltpu.VMEM((nz, rs) + blk, BF),
            pltpu.VMEM((nz + 1, rs) + blk, BF),
            pltpu.VMEM((level, cs) + blk, BF),
            pltpu.VMEM((n_row, kr, cs) + blk, BF),
            pltpu.VMEM(blk, BF),
            pltpu.VMEM((n_row,) + blk, BF),
            pltpu.VMEM((max(rs, kr * cs),) + blk, F32),
            pltpu.VMEM(blk, F32),
            dma((3,)), dma((n_row,)), dma((n_row,)), dma((n_row,)),
            dma((nz + 1,)), dma((nz + 1,)), dma((nz, 2, 2)), dma((nz, 2)),
            dma((nz, hp)), dma((nz, hp)), dma((nz, hp)), dma((nz + 1, hp)),
            dma((n_col,)), dma((n_row, kr)), dma((n_row,)), dma((n_row,)),
        ],
        compiler_params=pltpu.CompilerParams(
            collective_id=0, has_side_effects=True, vmem_limit_bytes=60 * 1024 * 1024
        ),
    )(members, ancestor_inv, lower_panel, upper_panel, pivot_inv)


def solution(mesh):
    return jax.shard_map(
        body,
        mesh=mesh,
        in_specs=(
            P("row", "col", None, None),
            P("row", "col", None, None),
            P("col", "row", None, None),
            P("col", None, None),
            P(),
        ),
        out_specs=(P("col", "row", None, None), P("row", "col", None, None), P("col", None, None)),
        check_vma=False,
    )
```

```python
import functools

import jax
import jax.numpy as jnp
from jax import lax
from jax.experimental import pallas as pl
from jax.experimental.pallas import tpu as pltpu
from jax.sharding import PartitionSpec as P

NY = 2
CORES = 2
BF = jnp.bfloat16
F32 = jnp.float32


def kernel(
    n_row, n_col, nq, hp,
    mem, anc, low, upp, piv,
    low_out, upp_out, diag_out,
    a, lbuf, ubuf, pl_buf, yr, zr, pu, ur, ds, dr, acc, dacc,
    loc, l_s, l_rel, l_r, uy_s, uy_r, uz_s, uz_r, ry_s, ry_r, rz_s, rz_r, pu_s, pu_r, d_s, d_r,
):
    row = lax.axis_index("row")
    col = lax.axis_index("col")
    nz = n_col // NY
    nx = n_row // CORES
    x, core = row // CORES, row % CORES
    z, y = col // NY, col % NY
    yp = z * NY + (1 - y)
    rb, cb = anc.shape[0], anc.shape[1]
    kr, cs = low.shape[0], low.shape[1]
    rs = upp.shape[1]
    ny_blocks = rs - nq
    hb = rs // hp
    partner = x * CORES + (1 - core)

    def remote(src, dst, ss, rsem, **where):
        return pltpu.make_async_remote_copy(
            src_ref=src, dst_ref=dst, send_sem=ss, recv_sem=rsem, device_id=where
        )

    ca = pltpu.make_async_copy(anc, a, loc.at[0])
    cl = pltpu.make_async_copy(low, lbuf.at[pl.ds(row * kr, kr)], loc.at[1])
    cu = pltpu.make_async_copy(upp.at[0], ubuf.at[col], loc.at[2])
    cl.start()
    cu.start()
    ca.start()

    bar = pltpu.get_barrier_semaphore()
    for dx in range(1, n_row):
        pl.semaphore_signal(bar, inc=1, device_id={"row": (row + dx) % n_row})
    pl.semaphore_signal(bar, inc=1, device_id={"col": yp})

    @pl.when(z > 0)
    def _():
        pl.semaphore_signal(bar, inc=1, device_id={"col": col - NY})

    @pl.when(z < nz - 1)
    def _():
        pl.semaphore_signal(bar, inc=1, device_id={"col": col + NY})

    peers = n_row + jnp.where(z > 0, 1, 0) + jnp.where(z < nz - 1, 1, 0)
    pl.semaphore_wait(bar, peers)

    def l_own(r2):
        return remote(low, lbuf.at[pl.ds(row * kr, kr)], l_s.at[r2], l_r.at[row], row=r2)

    def l_recv(r2):
        blk = lbuf.at[pl.ds(r2 * kr, kr)]
        return remote(blk, blk, l_rel.at[r2], l_r.at[r2], row=partner)

    def uy_own(kind):
        part = pl.ds(0, ny_blocks) if kind else pl.ds(ny_blocks, nq)
        return remote(
            upp.at[0, part], ubuf.at[col, part], uy_s.at[nz if kind == 0 else z],
            uy_r.at[nz if kind == 0 else z], col=yp,
        )

    def uy_got(kind, zs):
        part = pl.ds(0, ny_blocks) if kind else pl.ds(ny_blocks, nq)
        blk = ubuf.at[zs * NY + (1 - y), part]
        return remote(blk, blk, uy_s.at[zs], uy_r.at[nz if kind == 0 else zs], col=yp)

    def uy_pass(zs):
        blk = ubuf.at[zs * NY + y, pl.ds(0, ny_blocks)]
        return remote(blk, blk, uy_s.at[zs], uy_r.at[zs], col=yp)

    def uz(zs, kind, up):
        if kind == 0:
            blk = ubuf.at[zs * NY + y]
        else:
            blk = ubuf.at[zs * NY + (1 - y), pl.ds(ny_blocks, nq)]
        to = col + NY if up else col - NY
        return remote(blk, blk, uz_s.at[zs, int(up), kind], uz_r.at[zs, kind], col=to)

    def uz_own(up):
        to = col + NY if up else col - NY
        return remote(upp.at[0], ubuf.at[col], uz_s.at[z, int(up), 0], uz_r.at[z, 0], col=to)

    def ry(zd, h):
        part = pl.ds(h * hb, hb)
        return remote(
            pl_buf.at[zd * NY + (1 - y), part], yr.at[zd, part], ry_s.at[zd, h], ry_r.at[zd, h],
            col=yp,
        )

    def rz(zd, h, up):
        part = pl.ds(h * hb, hb)
        slot = zd + 1 if up else zd
        to = col + NY if up else col - NY
        return remote(
            pl_buf.at[zd * NY + y, part], zr.at[slot, part], rz_s.at[zd, h], rz_r.at[slot, h],
            col=to,
        )

    def pu_copy(k):
        return remote(pu.at[k], ur.at[row, k % kr], pu_s.at[k], pu_r.at[row, k % kr], row=k // kr)

    def pu_got(r2, p):
        return remote(pu.at[0], ur.at[r2, p], pu_s.at[0], pu_r.at[r2, p], row=r2)

    def d_copy(r2):
        return remote(ds, dr.at[row], d_s.at[r2], d_r.at[row], row=r2)

    def d_got(r2):
        return remote(ds, dr.at[r2], d_s.at[r2], d_r.at[r2], row=r2)

    def d_relay(x2):
        r2 = x2 * CORES + core
        blk = dr.at[r2]
        return remote(blk, blk, d_s.at[x2 * CORES + 1 - core], d_r.at[r2], row=partner)

    def each_dir(fn):
        @pl.when(z > 0)
        def _():
            fn(False)

        @pl.when(z < nz - 1)
        def _():
            fn(True)

    def row_member(k, i):
        m = mem[k, row * rs + i]
        return m >= 0, jnp.clip(m - row * rb, 0, rb - 1)

    def col_member(k, j):
        m = mem[k, col * cs + j]
        return m >= 0, jnp.clip(m - col * cb, 0, cb - 1)

    zero = jnp.zeros((), BF)

    def lower_part(k):
        cols = [col_member(k, j) for j in range(cs)]
        panels = [jnp.where(cols[j][0], lbuf[k, j], zero) for j in range(cs)]

        def one(i, _):
            ok, ri = row_member(k, i)
            tot = None
            for j in range(cs):
                t = jnp.dot(a[ri, cols[j][1]], panels[j], preferred_element_type=F32)
                tot = t if tot is None else tot + t
            pl_buf[k, i] = jnp.where(ok, tot, 0.0).astype(BF)
            return 0

        lax.fori_loop(0, rs, one, 0)

    def upper_part(k):
        rows = [row_member(k, i) for i in range(rs)]

        def one(j, _):
            ok, cj = col_member(k, j)
            tot = None
            for i in range(rs):
                t = jnp.dot(
                    jnp.where(rows[i][0], ubuf[k, i], zero), a[rows[i][1], cj],
                    preferred_element_type=F32,
                )
                tot = t if tot is None else tot + t
            pu[k, j] = jnp.where(ok, tot, 0.0).astype(BF)
            return 0

        lax.fori_loop(0, cs, one, 0)

        @pl.when(k // kr != row)
        def _():
            pu_copy(k).start()

    def lower_group(r2):
        def one(p, _):
            k = r2 * kr + (p + 1 - y) % NY
            lower_part(k)

            @pl.when(k % NY != y)
            def _():
                for h in range(hp):
                    ry(k // NY, h).start()

            return 0

        lax.fori_loop(0, kr, one, 0)

    def target(t):
        x2 = (x + t // CORES) % nx
        q = t % CORES
        return x2 * CORES + jnp.where(2 * x2 >= nx, CORES - 1 - q, q)

    def both_groups(x2):
        def one(q, _):
            lower_group(x2 * CORES + jnp.where(2 * x2 >= nx, CORES - 1 - q, q))
            return 0

        lax.fori_loop(0, CORES, one, 0)

    l_own(partner).start()
    for dx in range(1, nx):
        l_own(((x + dx) % nx) * CORES + core).start()
    uy_own(0).start()
    each_dir(lambda up: uz_own(up).start())

    ca.wait()
    cl.wait()
    l_recv(partner).wait_recv()
    both_groups(x)

    uy_got(0, z).wait_recv()
    each_dir(lambda up: uz(z, 1, up).start())
    cu.wait()
    upper_part(col)

    def others(fn):
        for dx in range(1, nx):
            fn((x + dx) % nx)

    def relay(x2):
        l_recv(x2 * CORES + core).wait_recv()
        l_recv(x2 * CORES + core).start()

    others(relay)

    def by_side(d, fn):
        @pl.when(z - d >= 0)
        def _():
            fn(z - d, True)

        @pl.when(z + d <= nz - 1)
        def _():
            fn(z + d, False)

    def take(zs, up):
        for kind in range(2):
            uz(zs, kind, up).wait_recv()

            @pl.when((z < nz - 1) if up else (z > 0))
            def _():
                uz(zs, kind, up).start()

    by_side(1, take)

    def late(x2):
        l_recv(x2 * CORES + 1 - core).wait_recv()
        both_groups(x2)

    others(late)
    uy_own(1).start()
    by_side(1, lambda zs, up: uy_pass(zs).start())

    def near(d):
        def one(s, _):
            zs = z + (2 * s - 1) * d

            @pl.when(jnp.logical_and(zs >= 0, zs < nz))
            def _():
                upper_part(zs * NY + y)

            return 0

        lax.fori_loop(0, 2, one, 0)

    def far(d):
        def one(s, _):
            zs = z + (2 * s - 1) * d

            @pl.when(jnp.logical_and(zs >= 0, zs < nz))
            def _():
                uy_got(1, zs).wait_recv()
                upper_part(zs * NY + (1 - y))

            return 0

        lax.fori_loop(0, 2, one, 0)

    def band_sum(zd, t):
        k = zd * NY + y

        def go(up):
            def piece(h, _):
                part = pl.ds(h * hb, hb)
                ry(zd, h).wait_recv()

                @pl.when((z > 0) if up else (z < nz - 1))
                def _():
                    rz(zd, h, up).wait_recv()
                    slot = zd + 1 if up else zd
                    pl_buf[k, part] = (
                        pl_buf[k, part].astype(F32) + yr[zd, part].astype(F32)
                        + zr[slot, part].astype(F32)
                    ).astype(BF)

                @pl.when((z == 0) if up else (z == nz - 1))
                def _():
                    pl_buf[k, part] = (
                        pl_buf[k, part].astype(F32) + yr[zd, part].astype(F32)
                    ).astype(BF)

                rz(zd, h, up).start()
                return 0

            lax.fori_loop(0, hp, piece, 0)

        @pl.when(zd > z)
        def _():
            go(True)

        @pl.when(zd < z)
        def _():
            go(False)

    def chain(t):
        band_sum(target(t), t)

    near(1)
    edge = jnp.logical_or(z == 0, z == nz - 1)

    def take_pass(d):
        by_side(d, take)
        by_side(d, lambda zs, up: uy_pass(zs).start())
        near(d)

    def chains(t, _):
        chain(t)
        return 0

    @pl.when(edge)
    def _():
        lax.fori_loop(0, CORES, chains, 0)

    @pl.when(jnp.logical_not(edge))
    def _():
        def one(d, _):
            take_pass(d)
            return 0

        lax.fori_loop(2, nz - 1, one, 0)
        lax.fori_loop(0, CORES, chains, 0)

    @pl.when(edge)
    def _():
        def one(d, _):
            take_pass(d)
            chain(CORES + d - 2)
            return 0

        lax.fori_loop(2, nz, one, 0)

    @pl.when(jnp.logical_not(edge))
    def _():
        lax.fori_loop(CORES, nz, chains, 0)

    uy_got(1, z).wait_recv()
    upper_part(yp)
    far(1)

    def final(h, _):
        part = pl.ds(h * hb, hb)
        ry(z, h).wait_recv()
        acc[part] = pl_buf[col, part].astype(F32) + yr[z, part].astype(F32)

        @pl.when(z > 0)
        def _():
            rz(z, h, True).wait_recv()
            acc[part] = acc[part] + zr[z + 1, part].astype(F32)

        @pl.when(z < nz - 1)
        def _():
            rz(z, h, False).wait_recv()
            acc[part] = acc[part] + zr[z, part].astype(F32)

        low_out[0, part] = (-acc[part]).astype(BF)
        return 0

    lax.fori_loop(0, hp, final, 0)
    tot = None
    for i in range(rs):
        t = jnp.dot(
            jnp.where(row_member(col, i)[0], ubuf[col, i], zero), low_out[0, i],
            preferred_element_type=F32,
        )
        tot = t if tot is None else tot + t
    dacc[...] = tot
    ds[...] = tot.astype(BF)
    others(lambda x2: d_copy(x2 * CORES + core).start())
    d_copy(partner).start()

    lax.fori_loop(2, nz, lambda d, _: (far(d), 0)[1], 0)

    def d_pass(x2):
        d_got(x2 * CORES + core).wait_recv()
        d_relay(x2).start()

    def d_add(r2):
        dacc[...] = dacc[...] + dr[r2].astype(F32)

    others(d_pass)
    d_got(partner).wait_recv()
    d_add(partner)

    def d_add_chip(x2):
        d_add(x2 * CORES + core)
        d_got(x2 * CORES + 1 - core).wait_recv()
        d_add(x2 * CORES + 1 - core)

    others(d_add_chip)
    diag_out[0] = piv[0] - dacc[...]

    for p in range(kr):
        for j in range(cs):
            acc[p * cs + j] = pu[row * kr + p, j].astype(F32)
    for dx in range(1, n_row):
        r2 = (row + dx) % n_row
        for p in range(kr):
            pu_got(r2, p).wait_recv()
            for j in range(cs):
                acc[p * cs + j] = acc[p * cs + j] + ur[r2, p, j].astype(F32)
    for p in range(kr):
        for j in range(cs):
            upp_out[p, j] = (-acc[p * cs + j]).astype(BF)

    l_own(partner).wait_send()
    for dx in range(1, nx):
        r2 = ((x + dx) % nx) * CORES + core
        l_own(r2).wait_send()
        l_recv(r2).wait_send()
    uy_own(0).wait_send()
    uy_own(1).wait_send()

    def own_done(up):
        uz_own(up).wait_send()
        uz(z, 1, up).wait_send()

    each_dir(own_done)

    def passed(zs, up):
        uy_pass(zs).wait_send()

        @pl.when((z < nz - 1) if up else (z > 0))
        def _():
            for kind in range(2):
                uz(zs, kind, up).wait_send()

    for d in range(1, nz):
        by_side(d, passed)

    def sums_done(zd, _):
        for h in range(hp):
            ry(zd, h).wait_send()

            @pl.when(zd > z)
            def _():
                rz(zd, h, True).wait_send()

            @pl.when(zd < z)
            def _():
                rz(zd, h, False).wait_send()

        return 0

    lax.fori_loop(0, nz, sums_done, 0)

    def parts_done(k, _):
        @pl.when(k // kr != row)
        def _():
            pu_copy(k).wait_send()

        return 0

    lax.fori_loop(0, n_col, parts_done, 0)
    d_copy(partner).wait_send()

    def d_done(x2):
        d_copy(x2 * CORES + core).wait_send()
        d_relay(x2).wait_send()

    others(d_done)


def hand_over(*refs):
    for src, dst in zip(refs[:3], refs[3:]):
        dst[...] = src[...]


def body(ancestor_inv, lower_panel, upper_panel, pivot_inv, members):
    n_col = lax.axis_size("col")
    n_row = lax.axis_size("row")
    side = ancestor_inv.shape[2]
    rb, cb = ancestor_inv.shape[:2]
    kr, cs = lower_panel.shape[:2]
    per_col, rs = upper_panel.shape[:2]
    level = members.shape[0]
    nz = n_col // NY
    assert per_col == 1 and level == n_col and kr == NY and nz == n_row
    hp = 2
    nq = rs // 2
    blk = (side, side)
    dma = pltpu.SemaphoreType.DMA
    vmem = pl.BlockSpec(memory_space=pltpu.VMEM)
    hbm = pl.BlockSpec(memory_space=pltpu.HBM)
    held = rb * cb + 3 * level * cs + 2 * n_col * rs + (2 * nz + 1) * rs + n_row * (kr * cs + 1)
    limit = 2 * side * side * (held + 32)
    outs = pl.pallas_call(
        functools.partial(kernel, n_row, n_col, nq, hp),
        out_shape=(
            jax.ShapeDtypeStruct((per_col, rs) + blk, BF),
            jax.ShapeDtypeStruct((kr, cs) + blk, BF),
            jax.ShapeDtypeStruct((per_col,) + blk, F32),
        ),
        in_specs=[pl.BlockSpec(memory_space=pltpu.SMEM), hbm, hbm, hbm, vmem],
        out_specs=(vmem, vmem, vmem),
        scratch_shapes=[
            pltpu.VMEM((rb, cb) + blk, BF),
            pltpu.VMEM((level, cs) + blk, BF),
            pltpu.VMEM((n_col, rs) + blk, BF),
            pltpu.VMEM((n_col, rs) + blk, BF),
            pltpu.VMEM((nz, rs) + blk, BF),
            pltpu.VMEM((nz + 1, rs) + blk, BF),
            pltpu.VMEM((level, cs) + blk, BF),
            pltpu.VMEM((n_row, kr, cs) + blk, BF),
            pltpu.VMEM(blk, BF),
            pltpu.VMEM((n_row,) + blk, BF),
            pltpu.VMEM((max(rs, kr * cs),) + blk, F32),
            pltpu.VMEM(blk, F32),
            dma((3,)), dma((n_row,)), dma((n_row,)), dma((n_row,)),
            dma((nz + 1,)), dma((nz + 1,)), dma((nz, 2, 2)), dma((nz, 2)),
            dma((nz, hp)), dma((nz, hp)), dma((nz, hp)), dma((nz + 1, hp)),
            dma((n_col,)), dma((n_row, kr)), dma((n_row,)), dma((n_row,)),
        ],
        compiler_params=pltpu.CompilerParams(
            collective_id=0, has_side_effects=True, vmem_limit_bytes=60 * 1024 * 1024
        ),
    )(members, ancestor_inv, lower_panel, upper_panel, pivot_inv)
    return pl.pallas_call(
        hand_over,
        out_shape=tuple(jax.ShapeDtypeStruct(o.shape, o.dtype) for o in outs),
        in_specs=[vmem] * 3,
        out_specs=(vmem,) * 3,
    )(*outs)


def solution(mesh):
    return jax.shard_map(
        body,
        mesh=mesh,
        in_specs=(
            P("row", "col", None, None),
            P("row", "col", None, None),
            P("col", "row", None, None),
            P("col", None, None),
            P(),
        ),
        out_specs=(P("col", "row", None, None), P("row", "col", None, None), P("col", None, None)),
        check_vma=False,
    )
```
